256 devices in a mesh: parts: 2 (over y), samp: 128 (over z, x, core).
Axes of the slice: x: 4, y: 2, z: 16, core: 2. Of those that a mesh axis runs over, the one named last changes fastest.
The devices are a block of a 4x16x16 slice.
Arguments:
- expression: bfloat16 [8192, 20480], P(('parts', 'samp')), parts along dimension 0, may hold values from -24 to 24
- current: bfloat16 [8192, 256], P(('parts', 'samp')), parts along dimension 0, may hold values from -6 to 6
- next_packed: int32 [512, 256], P(('parts', 'samp')), parts along dimension 0, may hold values from -2147483648 to 1789569706, as said below
- covariates: float32 [8192, 64], P(('parts', 'samp')), parts along dimension 0, may hold values from -1 to 1
Outputs:
- scores: float32 [40960, 256], P(('parts', 'samp')), parts along dimension 0
- next_block: bfloat16 [8192, 256], P(('parts', 'samp')), parts along dimension 0
The draws below stay inside these ranges and needn't reach their ends.
There are 2 independent parts, one for each index of `parts`. The reference program is written for one: setup_inputs(seed, part) draws one part's arguments, and reference() takes and returns one part's arrays. A program takes and returns all parts, laid end to end along the dimension named above; each array names one. Nothing has to cross between parts.
Inputs may be any that keep to these rules, and one draw needn't show every extreme that they name: Each word holds the dosages (0, 1 or 2) of 16 consecutive samples of one variant, two bits a sample: sample 16 w + j of variant v in bits 2 j and 2 j + 1 of next_packed[v, w], bit 31 being the sign bit of the int32 word.
All inputs are finite; a program needn't handle non-finite values.
Results may differ from the reference program's by a relative error of at most 0.0004.
Values may be sent and summed in bfloat16 or wider, within the bound.
No kernel may reach another device: no remote copies, remote signals or barrier semaphores. Data moves between devices by JAX's collectives and lax.ppermute only.
A program may use at most 64 MiB of HBM per device.

```python
import jax
import jax.numpy as jnp
from jax import lax

GENES = 20480
VARS = 256
COVS = 64
SAMPLES = 4096


def draw_next_packed(key, part):
    base = jax.random.fold_in(key, 11)
    key_freq, key_first, key_second = jax.random.split(base, 3)
    word_count = SAMPLES // 16
    allele = jax.random.randint(key_freq, (VARS, 1, 1), 200, 1001, dtype=jnp.int32)
    sample_index = 16 * jnp.arange(word_count, dtype=jnp.int32)[None, :, None] + jnp.arange(16, dtype=jnp.int32)[None, None, :]
    thresh = allele * (100 + 400 * sample_index // SAMPLES) // 1000
    first = jax.random.randint(key_first, (VARS, word_count, 16), 0, 1000, dtype=jnp.int32)
    second = jax.random.randint(key_second, (VARS, word_count, 16), 0, 1000, dtype=jnp.int32)
    dose = (first < thresh).astype(jnp.int32) + (second < thresh).astype(jnp.int32)
    shifts = 2 * jnp.arange(16, dtype=jnp.int32)
    return jnp.sum(lax.shift_left(dose, shifts[None, None, :]), axis=2, dtype=jnp.int32)


def draw_covariates(key, part):
    base = jax.random.fold_in(key, 7)
    key_noise, key_phase = jax.random.split(base, 2)
    noise = jax.random.normal(key_noise, (SAMPLES, COVS), jnp.float32)
    noise = noise * float(SAMPLES) ** (-0.5)
    phase = jax.random.uniform(key_phase, (COVS,), jnp.float32, 0.0, 6.2831853)
    column = jnp.arange(COVS, dtype=jnp.int32)
    freq = (column % 8 + 1).astype(jnp.float32)
    position = (jnp.arange(SAMPLES, dtype=jnp.float32) + 0.5) / SAMPLES
    smooth = jnp.cos(3.14159265 * freq[None, :] * position[:, None] + phase[None, :]) * (2.0 / SAMPLES) ** 0.5
    return jnp.where((column < 8)[None, :], 0.5 * noise + 0.85 * smooth, noise)


def spiked(result, stream_key, source, target, blocks, factor):
    owner, partner = [(jnp.arange(result.shape[dim]) // (result.shape[dim] // blocks)).reshape([-1 if axis == dim else 1 for axis in range(result.ndim)]) for dim in (source, target)]
    chosen = jax.random.permutation(stream_key, blocks)[partner]
    strong = (owner == chosen) | (owner == (partner + blocks // 2) % blocks)
    return jnp.where(strong, factor * result, result)


def block_scale(stream_key, extent, cuts, low, largest):
    level, own = 1.0, jax.random.fold_in(stream_key, 6)
    for dim, parts in cuts:
        draws = jnp.exp(jax.random.uniform(jax.random.fold_in(own, dim), (parts,), jnp.float32, low / len(cuts), largest / len(cuts)))
        level = level * jnp.repeat(draws, extent[dim] // parts).reshape([-1 if axis == dim else 1 for axis in range(len(extent))])
    return level


def scatter_about(rng, dims, spread, most, pieces=(), kind=jnp.bfloat16):
    loudness = block_scale(rng, dims, pieces, -0.22, 0.18) if pieces else 1.0
    result = jax.random.normal(rng, dims, jnp.float32) * spread * loudness
    return jnp.minimum(jnp.maximum(result, -most), most).astype(kind)


def bell_draw_with(stream_key, dims, deviation, limit, cuts, heavy, held_as=jnp.bfloat16):
    drawn = deviation * jax.random.normal(stream_key, dims, jnp.float32)
    if cuts:
        drawn = drawn * block_scale(stream_key, dims, cuts, -0.22, 0.18)
    return jnp.clip(spiked(drawn, jax.random.fold_in(stream_key, 3), *heavy), -limit, limit).astype(held_as)


def setup_inputs(seed: int = 0, part: int = 0) -> dict:
    seeds = jax.random.split(jax.random.key(seed), 5)
    own_keys = jax.random.split(jax.random.fold_in(seeds[4], part), 5)
    expression = bell_draw_with(own_keys[0], (SAMPLES, GENES), 1.0, 24.0, ((0, 128),), (0, 1, 128, 5.5))
    current = scatter_about(own_keys[1], (SAMPLES, VARS), 1.0, 6.0, ((0, 128),))
    next_packed = draw_next_packed(jax.random.fold_in(jax.random.fold_in(seeds[4], part), 71), part)
    covariates = draw_covariates(jax.random.fold_in(jax.random.fold_in(seeds[4], part), 71), part)
    return dict(expression=expression, current=current, next_packed=next_packed, covariates=covariates)


def unpack_words(packed_words):
    shifts = 2 * jnp.arange(16, dtype=jnp.int32)
    fields = jnp.bitwise_and(lax.shift_right_logical(packed_words[:, :, None], shifts[None, None, :]), 3)
    return fields.reshape(packed_words.shape[0], -1).T.astype(jnp.float32)

def reference(expression, current, next_packed, covariates):
    scale_factor = float(SAMPLES) ** (-0.5)
    scores = lax.dot_general(expression, current, (((0,), (0,)), ((), ())), preferred_element_type=jnp.float32) * scale_factor
    dosage = unpack_words(next_packed)
    average = lax.optimization_barrier(jnp.sum(dosage, axis=0)) / SAMPLES
    projected = lax.dot_general(covariates, dosage, (((0,), (0,)), ((), ())), precision=lax.Precision.HIGHEST)
    cov_sums = lax.optimization_barrier(jnp.sum(covariates, axis=0))
    loading = projected - cov_sums[:, None] * average[None, :]
    leftover = dosage - average[None, :] - jnp.dot(covariates, loading, precision=lax.Precision.HIGHEST)
    sq_norm = lax.optimization_barrier(jnp.sum(leftover * leftover, axis=0))
    next_block = (leftover * lax.rsqrt(sq_norm / SAMPLES + 1e-05)[None, :]).astype(jnp.bfloat16)
    return (scores, next_block)
```

```python
import jax
import jax.numpy as jnp
from jax import lax
from jax.experimental import pallas as pl
from jax.experimental.pallas import tpu as pltpu
from jax.sharding import Mesh
from jax.sharding import PartitionSpec as P

RING = 8
LOCAL = 16
SPEC = P(("parts", "q", "j"), None)
F32 = jnp.float32
BF16 = jnp.bfloat16
HIGHEST = lax.Precision.HIGHEST
WORD = 16


def dot(left, right, dims, precision=None):
    return lax.dot_general(
        left, right, (dims, ((), ())), precision=precision, preferred_element_type=F32
    )


def small_kernel(current_ref, covariates_ref, packed_ref, small_ref, words_ref):
    rows, variants = current_ref.shape
    covs = covariates_ref.shape[1]
    cov = covariates_ref[...]
    high = cov.astype(BF16)
    rest = cov - high.astype(F32)
    mid = rest.astype(BF16)
    low = (rest - mid.astype(F32)).astype(BF16)
    own = jnp.concatenate([current_ref[...], high, mid, low, jnp.zeros_like(low)], axis=1)
    for j in range(LOCAL):
        small_ref[j * rows : (j + 1) * rows, :] = own
    held, words = packed_ref.shape
    share = words // RING
    words_ref[...] = jnp.zeros_like(words_ref)
    packed = packed_ref[...]
    for q in range(RING):
        words_ref[q * 8 : q * 8 + held, 0:share] = packed[:, q * share : (q + 1) * share]


def regroup_kernel(expression_ref, out_ref):
    rows, genes = expression_ref.shape
    share = genes // (RING * LOCAL)
    for j in range(LOCAL):
        pieces = []
        for q in range(RING):
            at = (q * LOCAL + j) * share
            pieces.append(expression_ref[:, at : at + share])
        out_ref[j * rows : (j + 1) * rows, :] = jnp.concatenate(pieces, axis=1)


def unpack(words_ref, held, share):
    words = jnp.concatenate([words_ref[q * 8 : q * 8 + held, 0:share] for q in range(RING)], axis=0)
    wide = jnp.concatenate([words] * 4, axis=1)
    lane = lax.broadcasted_iota(jnp.int32, wide.shape, 1)
    octets = (lax.shift_right_logical(wide, 8 * (lane // share)) & 255).astype(F32).astype(BF16)
    samples = share * WORD
    row = lax.broadcasted_iota(jnp.int32, (4 * share, samples), 0)
    col = lax.broadcasted_iota(jnp.int32, (4 * share, samples), 1)
    pick = (row % share == col // WORD) & (row // share == (col % WORD) // 4)
    spread = dot(octets, pick.astype(F32).astype(BF16), ((1,), (0,))).astype(jnp.int32)
    place = lax.broadcasted_iota(jnp.int32, spread.shape, 1)
    return (lax.shift_right_logical(spread, 2 * (place % 4)) & 3).astype(F32)


def covariate_terms(small_ref, variants, covs):
    return [small_ref[:, variants + k * covs : variants + (k + 1) * covs] for k in range(3)]


def stats_kernel(held, share, variants, covs, small_ref, words_ref, out_ref):
    dosage = unpack(words_ref, held, share)
    count, samples = dosage.shape
    ones = jnp.ones((8, samples), F32)
    wide = jnp.concatenate([dosage, ones], axis=0)
    exact = wide.astype(BF16)
    terms = covariate_terms(small_ref, variants, covs)
    projected = sum(dot(exact, term, ((1,), (0,))) for term in reversed(terms))
    out_ref[...] = jnp.zeros_like(out_ref)
    out_ref[0 : count + 8, 0:covs] = projected
    out_ref[0 : count + 8, covs : covs + 1] = jnp.sum(wide, axis=1, keepdims=True)
    out_ref[0 : count + 8, covs + 1 : covs + 2] = jnp.sum(wide * wide, axis=1, keepdims=True)
    cov = sum(term.astype(F32) for term in reversed(terms))
    gram = dot(cov, cov, ((0,), (0,)), HIGHEST)
    half = covs // 2
    out_ref[count + 8 : count + 8 + half, 0:covs] = gram[0:half]
    out_ref[count + 8 : count + 8 + half, covs : 2 * covs] = gram[half:]


def finish_kernel(
    held, share, variants, covs, total, where_ref, small_ref, words_ref, *refs
):
    sums = refs[:-1]
    out_ref = refs[-1]
    dosage = unpack(words_ref, held, share)
    count, samples = dosage.shape
    table = sums[0][...]
    for ref in sums[1:]:
        table = table + ref[...]
    half = covs // 2
    gram = jnp.concatenate(
        [
            table[count + 8 : count + 8 + half, 0:covs],
            table[count + 8 : count + 8 + half, covs : 2 * covs],
        ],
        axis=0,
    )
    projected = table[0:count, 0:covs]
    cov_sums = table[count : count + 1, 0:covs]
    counted = table[0:count, covs : covs + 1]
    squares = table[0:count, covs + 1 : covs + 2]
    average = counted / total
    loading = projected - average * cov_sums
    through = dot(loading, gram, ((1,), (0,)), HIGHEST)
    sq_norm = (
        squares
        - counted * average
        + jnp.sum(loading * (through - 2.0 * loading), axis=1, keepdims=True)
    )
    cov = sum(term.astype(F32) for term in reversed(covariate_terms(small_ref, variants, covs)))
    leftover = dosage - average - dot(loading, cov, ((1,), (1,)), HIGHEST)
    scaled = (leftover * lax.rsqrt(sq_norm / total + 1e-05)).astype(BF16)
    row = lax.broadcasted_iota(jnp.int32, (count, variants), 0)
    col = lax.broadcasted_iota(jnp.int32, (count, variants), 1)
    target = (row // held) * (held * LOCAL) + where_ref[0] * held + row % held
    place = (col == target).astype(F32).astype(BF16)
    out_ref[...] = dot(scaled, place, ((0,), (0,))).astype(BF16)


def shift(array, by):
    return lax.ppermute(array, "q", [(k, (k + by) % RING) for k in range(RING)])


def shards(expression, current, next_packed, covariates):
    rows, genes = expression.shape
    variants = current.shape[1]
    covs = covariates.shape[1]
    held, words = next_packed.shape
    share = words // RING
    total = rows * RING * LOCAL
    own_genes = genes // (RING * LOCAL)
    q = lax.axis_index("q")
    j = lax.axis_index("j")

    small, packed = pl.pallas_call(
        small_kernel,
        out_shape=(
            jax.ShapeDtypeStruct((LOCAL * rows, variants + 4 * covs), BF16),
            jax.ShapeDtypeStruct((RING * 8, 128), jnp.int32),
        ),
    )(current, covariates, next_packed)
    packed = lax.all_to_all(packed, "q", split_axis=0, concat_axis=0, tiled=True)
    small = lax.all_to_all(small, "j", split_axis=0, concat_axis=0, tiled=True)
    regrouped = pl.pallas_call(
        regroup_kernel,
        out_shape=jax.ShapeDtypeStruct((LOCAL * rows, genes // LOCAL), BF16),
    )(expression)
    regrouped = lax.all_to_all(regrouped, "j", split_axis=0, concat_axis=0, tiled=True)

    def stats_body(*refs):
        stats_kernel(held, share, variants, covs, *refs)

    count = RING * held
    stats = pl.pallas_call(
        stats_body, out_shape=jax.ShapeDtypeStruct((count + 8 + covs // 2, 2 * covs), F32)
    )(small, packed)
    sums = [stats]
    right, left = stats, stats
    for step in range(RING // 2):
        right = shift(right, 1)
        sums.append(right)
        if step < RING // 2 - 1:
            left = shift(left, -1)
            sums.append(left)

    def finish_body(*refs):
        finish_kernel(held, share, variants, covs, float(total), *refs)

    placed = pl.pallas_call(
        finish_body,
        out_shape=jax.ShapeDtypeStruct((LOCAL * rows, variants), BF16),
        in_specs=[pl.BlockSpec(memory_space=pltpu.SMEM)]
        + [pl.BlockSpec(memory_space=pltpu.VMEM)] * (2 + len(sums)),
    )(j.reshape(1).astype(jnp.int32), small, packed, *sums)
    placed = lax.all_to_all(placed, "j", split_axis=0, concat_axis=0, tiled=True)
    next_block = jnp.sum(placed.reshape(LOCAL, rows, variants).astype(F32), axis=0).astype(BF16)

    scale_factor = float(total) ** (-0.5)
    partial = dot(regrouped, small[:, :variants], ((0,), (0,))).reshape(RING, own_genes, variants)

    def block(away):
        return lax.dynamic_index_in_dim(partial, (q + away) % RING, 0, keepdims=False)

    far = RING // 2
    cut = own_genes // 2
    opposite = block(far)
    right, left = shift(opposite[:cut], 1), shift(opposite[cut:], -1)
    for away in range(far - 1, 0, -1):
        ahead, behind = block(away), block(-away)
        if away == far - 1:
            ahead = jnp.concatenate([ahead[:cut] + right, ahead[cut:]], axis=0)
            behind = jnp.concatenate([behind[:cut], behind[cut:] + left], axis=0)
        else:
            ahead, behind = ahead + right, behind + left
        right, left = shift(ahead, 1), shift(behind, -1)
    scores = (block(0) + right + left) * scale_factor
    return (scores, next_block)


def solution(mesh):
    split = Mesh(mesh.devices.reshape(mesh.shape["parts"], RING, LOCAL), ("parts", "q", "j"))
    return jax.shard_map(
        shards, mesh=split, in_specs=(SPEC,) * 4, out_specs=(SPEC,) * 2, check_vma=False
    )
```

```python
import functools

import jax
import jax.numpy as jnp
from jax import lax
from jax.experimental import pallas as pl
from jax.experimental.pallas import tpu as pltpu
from jax.sharding import Mesh
from jax.sharding import PartitionSpec as P

RING = 8
LOCAL = 16
SPEC = P(("parts", "q", "j"), None)
F32 = jnp.float32
BF16 = jnp.bfloat16
HIGHEST = lax.Precision.HIGHEST
WORD = 16


def dot(left, right, dims, precision=None):
    return lax.dot_general(
        left, right, (dims, ((), ())), precision=precision, preferred_element_type=F32
    )


def prepare_kernel(expression_ref, current_ref, covariates_ref, packed_ref, out_ref, words_ref):
    rows, genes = expression_ref.shape
    share = genes // (RING * LOCAL)
    cov = covariates_ref[...]
    high = cov.astype(BF16)
    low = (cov - high.astype(F32)).astype(BF16)
    own = [current_ref[...], high, low]
    for j in range(LOCAL):
        pieces = []
        for q in range(RING):
            at = (q * LOCAL + j) * share
            pieces.append(expression_ref[:, at : at + share])
        out_ref[j * rows : (j + 1) * rows, :] = jnp.concatenate(pieces + own, axis=1)
    held, words = packed_ref.shape
    split = words // RING
    words_ref[...] = jnp.zeros_like(words_ref)
    packed = packed_ref[...]
    for q in range(RING):
        words_ref[q * 8 : q * 8 + held, 0:split] = packed[:, q * split : (q + 1) * split]


def product_kernel(genes, variants, where_ref, rows_ref, *refs):
    outs, whole_ref = refs[:-1], refs[-1]
    whole_ref[...] = dot(rows_ref[:, :genes], rows_ref[:, genes : genes + variants], ((0,), (0,)))
    share = genes // RING
    half = share // 2
    for ahead in range(RING):
        at = lax.rem(where_ref[1] + ahead, RING) * share
        for part in range(2):
            outs[2 * ahead + part][...] = whole_ref[pl.ds(at + part * half, half), :]


def total_kernel(scale, *refs):
    out_ref = refs[-1]
    half = refs[0].shape[0]
    for part in range(2):
        terms = [ref[...] for ref in refs[part:-1:2]]
        out_ref[part * half : (part + 1) * half, :] = sum(terms[1:], terms[0]) * scale


def unpack(position, word_refs, held, share):
    words = jnp.concatenate([ref[0:held, 0:share] for ref in word_refs], axis=0)
    wide = jnp.concatenate([words] * 4, axis=1)
    lane = lax.broadcasted_iota(jnp.int32, wide.shape, 1)
    octets = (lax.shift_right_logical(wide, 8 * (lane // share)) & 255).astype(F32).astype(BF16)
    count = RING * held
    row = lax.broadcasted_iota(jnp.int32, (count, count), 0)
    col = lax.broadcasted_iota(jnp.int32, (count, count), 1)
    behind = (position + RING - row // held) % RING
    order = (col // held == behind) & (col % held == row % held)
    octets = dot(order.astype(F32).astype(BF16), octets, ((1,), (0,))).astype(BF16)
    samples = share * WORD
    row = lax.broadcasted_iota(jnp.int32, (4 * share, samples), 0)
    col = lax.broadcasted_iota(jnp.int32, (4 * share, samples), 1)
    pick = (row % share == col // WORD) & (row // share == (col % WORD) // 4)
    spread = dot(octets, pick.astype(F32).astype(BF16), ((1,), (0,))).astype(jnp.int32)
    place = lax.broadcasted_iota(jnp.int32, spread.shape, 1)
    return (lax.shift_right_logical(spread, 2 * (place % 4)) & 3).astype(F32)


def covariate_terms(rows_ref, at, covs):
    return [rows_ref[:, at + k * covs : at + (k + 1) * covs] for k in range(2)]


def stats_kernel(held, share, at, covs, where_ref, rows_ref, *refs):
    out_ref = refs[RING]
    dosage = unpack(where_ref[1], refs[:RING], held, share)
    count, samples = dosage.shape
    ones = jnp.ones((8, samples), F32)
    wide = jnp.concatenate([dosage, ones], axis=0)
    exact = wide.astype(BF16)
    terms = covariate_terms(rows_ref, at, covs)
    projected = sum(dot(exact, term, ((1,), (0,))) for term in reversed(terms))
    half = covs // 2
    height = count + 8 + half
    cov = sum(term.astype(F32) for term in reversed(terms))
    gram = dot(cov, cov, ((0,), (0,)), HIGHEST)
    counted = jnp.sum(wide, axis=1, keepdims=True)
    squares = jnp.sum(wide * wide, axis=1, keepdims=True)
    pad = jnp.zeros((count + 8, covs - 2), F32)
    table = jnp.concatenate([projected, counted, squares, pad], axis=1)
    lower = jnp.concatenate([gram[0:half], gram[half:]], axis=1)
    out_ref[0 : count + 8, :] = table
    out_ref[count + 8 : height, :] = lower


def finish_kernel(held, share, at, variants, covs, total, where_ref, rows_ref, *refs):
    out_ref = refs[2 * RING]
    dosage = unpack(where_ref[1], refs[:RING], held, share)
    count, _ = dosage.shape
    half = covs // 2
    table = refs[RING][...]
    for ref in refs[RING + 1 : 2 * RING]:
        table = table + ref[...]
    gram = jnp.concatenate(
        [
            table[count + 8 : count + 8 + half, 0:covs],
            table[count + 8 : count + 8 + half, covs : 2 * covs],
        ],
        axis=0,
    )
    projected = table[0:count, 0:covs]
    cov_sums = table[count : count + 1, 0:covs]
    counted = table[0:count, covs : covs + 1]
    squares = table[0:count, covs + 1 : covs + 2]
    average = counted / total
    loading = projected - average * cov_sums
    through = dot(loading, gram, ((1,), (0,)), HIGHEST)
    sq_norm = (
        squares
        - counted * average
        + jnp.sum(loading * (through - 2.0 * loading), axis=1, keepdims=True)
    )
    cov = sum(term.astype(F32) for term in reversed(covariate_terms(rows_ref, at, covs)))
    leftover = dosage - average - dot(loading, cov, ((1,), (1,)), HIGHEST)
    scaled = (leftover * lax.rsqrt(sq_norm / total + 1e-05)).astype(BF16)
    row = lax.broadcasted_iota(jnp.int32, (count, variants), 0)
    col = lax.broadcasted_iota(jnp.int32, (count, variants), 1)
    target = (row // held) * (held * LOCAL) + where_ref[0] * held + row % held
    place = (col == target).astype(F32).astype(BF16)
    out_ref[...] = dot(scaled, place, ((0,), (0,))).astype(BF16)


def exchange(array, axis):
    return lax.all_to_all(array, axis, split_axis=0, concat_axis=0, tiled=True)


def shift(array, by):
    return lax.ppermute(array, "q", [(k, (k + by) % RING) for k in range(RING)])


def kernel(body, out_shape, given=(), scratch=()):
    specs = [pl.BlockSpec(memory_space=space) for space in given]

    def call(*operands):
        rest = operands[len(specs) :]
        held = [pltpu.with_memory_space_constraint(array, pltpu.VMEM) for array in rest]
        return pl.pallas_call(
            body,
            out_shape=out_shape,
            in_specs=specs + [pl.BlockSpec(memory_space=pltpu.VMEM)] * len(held),
            scratch_shapes=scratch,
        )(*operands[: len(specs)], *held)

    return call


def block_step(expression, current, next_packed, covariates):
    rows, genes = expression.shape
    variants = current.shape[1]
    covs = covariates.shape[1]
    held, words = next_packed.shape
    share = words // RING
    total = rows * RING * LOCAL
    own_genes = genes // (RING * LOCAL)
    q = lax.axis_index("q")
    j = lax.axis_index("j")

    count = RING * held
    height = count + 8 + covs // 2
    local_genes = genes // LOCAL
    at = local_genes + variants
    moved, packed = kernel(
        prepare_kernel,
        (
            jax.ShapeDtypeStruct((LOCAL * rows, at + 2 * covs), BF16),
            pltpu.VMEM((RING * 8, 128), jnp.int32),
        ),
        [pltpu.VMEM] * 4,
    )(expression, current, covariates, next_packed)
    moved = exchange(moved, "j")
    packed = packed.reshape(RING, 8, 128)
    pieces = []
    for ahead in range(RING):
        piece = lax.dynamic_index_in_dim(packed, (q + ahead) % RING, 0, keepdims=False)
        pieces.append(shift(piece, ahead) if ahead else piece)

    where = jnp.stack([j, q]).astype(jnp.int32)
    half = own_genes // 2
    blocks = kernel(
        functools.partial(product_kernel, local_genes, variants),
        [pltpu.VMEM((half, variants), F32)] * (2 * RING),
        [pltpu.SMEM],
        [pltpu.VMEM((local_genes, variants), F32)],
    )(where, moved)

    stats = kernel(
        functools.partial(stats_kernel, held, share, at, covs),
        jax.ShapeDtypeStruct((height, 2 * covs), F32),
        [pltpu.SMEM],
    )(where, moved, *pieces)
    sums = [stats]
    ahead, behind = stats, stats
    for hop in range(1, RING // 2 + 1):
        ahead = shift(ahead, 1)
        sums.append(ahead)
        if hop < RING // 2:
            behind = shift(behind, -1)
            sums.append(behind)
    placed = kernel(
        functools.partial(finish_kernel, held, share, at, variants, covs, float(total)),
        jax.ShapeDtypeStruct((LOCAL * rows, variants), BF16),
        [pltpu.SMEM],
    )(where, moved, *pieces, *sums)
    placed = exchange(placed, "j")
    next_block = jnp.sum(placed.reshape(LOCAL, rows, variants).astype(F32), axis=0).astype(BF16)

    scale_factor = float(total) ** (-0.5)
    far = RING // 2
    carried = {}
    for step in range(1, far + 1):
        for name, way, part, late in STREAMS:
            if step + late <= far:
                block = blocks[2 * (way * (far + 1 - step - late) % RING) + part]
                held_sum = carried[name] + block if name in carried else block
                carried[name] = shift(held_sum, way)
    scores = kernel(
        functools.partial(total_kernel, scale_factor),
        jax.ShapeDtypeStruct((own_genes, variants), F32),
    )(*blocks[:2], *(carried[name] for name in ("right_a", "right_b", "left_a", "left_b")))
    return (scores, next_block)


STREAMS = (("right_a", 1, 0, 0), ("left_b", -1, 1, 0), ("right_b", 1, 1, 1), ("left_a", -1, 0, 1))


def solution(mesh):
    split = Mesh(mesh.devices.reshape(mesh.shape["parts"], RING, LOCAL), ("parts", "q", "j"))
    return jax.shard_map(
        block_step, mesh=split, in_specs=(SPEC,) * 4, out_specs=(SPEC,) * 2, check_vma=False
    )
```

```python
import functools

import jax
import jax.numpy as jnp
from jax import lax
from jax.experimental import pallas as pl
from jax.experimental.pallas import tpu as pltpu
from jax.sharding import Mesh
from jax.sharding import PartitionSpec as P

RING = 8
LOCAL = 16
SPEC = P(("parts", "q", "j"), None)
F32 = jnp.float32
BF16 = jnp.bfloat16
HIGHEST = lax.Precision.HIGHEST
WORD = 16


def dot(left, right, dims, precision=None):
    return lax.dot_general(
        left, right, (dims, ((), ())), precision=precision, preferred_element_type=F32
    )


def regroup(expression_ref, out_ref, part, own):
    rows, genes = expression_ref.shape
    share = genes // (RING * LOCAL)
    half = share // 2
    for j in range(LOCAL):
        pieces = []
        for q in range(RING):
            first = (q * LOCAL + j) * share + part * half
            pieces.append(expression_ref[:, first : first + half])
        out_ref[j * rows : (j + 1) * rows, :] = jnp.concatenate(pieces + own, axis=1)


def first_kernel(expression_ref, current_ref, covariates_ref, packed_ref, out_ref, words_ref):
    cov = covariates_ref[...]
    high = cov.astype(BF16)
    low = (cov - high.astype(F32)).astype(BF16)
    regroup(expression_ref, out_ref, 0, [current_ref[...], high, low])
    held, words = packed_ref.shape
    split = words // RING
    words_ref[...] = jnp.zeros_like(words_ref)
    packed = packed_ref[...]
    for q in range(RING):
        words_ref[q * 8 : q * 8 + held, 0:split] = packed[:, q * split : (q + 1) * split]


def second_kernel(expression_ref, out_ref):
    regroup(expression_ref, out_ref, 1, [])


def product_kernel(genes, variants, at, where_ref, rows_ref, own_ref, *refs):
    outs, whole_ref = refs[:-1], refs[-1]
    whole_ref[...] = dot(rows_ref[:, :genes], own_ref[:, at : at + variants], ((0,), (0,)))
    half = genes // RING
    for ahead in range(RING):
        at = lax.rem(where_ref[1] + ahead, RING) * half
        outs[ahead][...] = whole_ref[pl.ds(at, half), :]


def total_kernel(scale, *refs):
    out_ref = refs[-1]
    half = refs[0].shape[0]
    for part in range(2):
        terms = [ref[...] for ref in refs[part:-1:2]]
        out_ref[part * half : (part + 1) * half, :] = sum(terms[1:], terms[0]) * scale


def unpack(position, word_refs, held, share):
    words = jnp.concatenate([ref[0:held, 0:share] for ref in word_refs], axis=0)
    wide = jnp.concatenate([words] * 4, axis=1)
    lane = lax.broadcasted_iota(jnp.int32, wide.shape, 1)
    octets = (lax.shift_right_logical(wide, 8 * (lane // share)) & 255).astype(F32).astype(BF16)
    count = RING * held
    row = lax.broadcasted_iota(jnp.int32, (count, count), 0)
    col = lax.broadcasted_iota(jnp.int32, (count, count), 1)
    behind = (position + RING - row // held) % RING
    order = (col // held == behind) & (col % held == row % held)
    octets = dot(order.astype(F32).astype(BF16), octets, ((1,), (0,))).astype(BF16)
    samples = share * WORD
    row = lax.broadcasted_iota(jnp.int32, (4 * share, samples), 0)
    col = lax.broadcasted_iota(jnp.int32, (4 * share, samples), 1)
    pick = (row % share == col // WORD) & (row // share == (col % WORD) // 4)
    spread = dot(octets, pick.astype(F32).astype(BF16), ((1,), (0,))).astype(jnp.int32)
    place = lax.broadcasted_iota(jnp.int32, spread.shape, 1)
    return (lax.shift_right_logical(spread, 2 * (place % 4)) & 3).astype(F32)


def covariate_terms(rows_ref, at, covs):
    return [rows_ref[:, at + k * covs : at + (k + 1) * covs] for k in range(2)]


def stats_kernel(held, share, at, covs, where_ref, rows_ref, *refs):
    out_ref = refs[RING]
    dosage = unpack(where_ref[1], refs[:RING], held, share)
    count, samples = dosage.shape
    ones = jnp.ones((8, samples), F32)
    wide = jnp.concatenate([dosage, ones], axis=0)
    exact = wide.astype(BF16)
    terms = covariate_terms(rows_ref, at, covs)
    projected = sum(dot(exact, term, ((1,), (0,))) for term in reversed(terms))
    half = covs // 2
    height = count + 8 + half
    cov = sum(term.astype(F32) for term in reversed(terms))
    gram = dot(cov, cov, ((0,), (0,)), HIGHEST)
    counted = jnp.sum(wide, axis=1, keepdims=True)
    squares = jnp.sum(wide * wide, axis=1, keepdims=True)
    pad = jnp.zeros((count + 8, covs - 2), F32)
    table = jnp.concatenate([projected, counted, squares, pad], axis=1)
    lower = jnp.concatenate([gram[0:half], gram[half:]], axis=1)
    out_ref[0 : count + 8, :] = table
    out_ref[count + 8 : height, :] = lower


def finish_kernel(held, share, at, variants, covs, total, where_ref, rows_ref, *refs):
    out_ref = refs[2 * RING]
    dosage = unpack(where_ref[1], refs[:RING], held, share)
    count, _ = dosage.shape
    half = covs // 2
    table = refs[RING][...]
    for ref in refs[RING + 1 : 2 * RING]:
        table = table + ref[...]
    gram = jnp.concatenate(
        [
            table[count + 8 : count + 8 + half, 0:covs],
            table[count + 8 : count + 8 + half, covs : 2 * covs],
        ],
        axis=0,
    )
    projected = table[0:count, 0:covs]
    cov_sums = table[count : count + 1, 0:covs]
    counted = table[0:count, covs : covs + 1]
    squares = table[0:count, covs + 1 : covs + 2]
    average = counted / total
    loading = projected - average * cov_sums
    through = dot(loading, gram, ((1,), (0,)), HIGHEST)
    sq_norm = (
        squares
        - counted * average
        + jnp.sum(loading * (through - 2.0 * loading), axis=1, keepdims=True)
    )
    cov = sum(term.astype(F32) for term in reversed(covariate_terms(rows_ref, at, covs)))
    leftover = dosage - average - dot(loading, cov, ((1,), (1,)), HIGHEST)
    scaled = (leftover * lax.rsqrt(sq_norm / total + 1e-05)).astype(BF16)
    row = lax.broadcasted_iota(jnp.int32, (count, variants), 0)
    col = lax.broadcasted_iota(jnp.int32, (count, variants), 1)
    target = (row // held) * (held * LOCAL) + where_ref[0] * held + row % held
    place = (col == target).astype(F32).astype(BF16)
    out_ref[...] = dot(scaled, place, ((0,), (0,))).astype(BF16)


def exchange(array, axis):
    return lax.all_to_all(array, axis, split_axis=0, concat_axis=0, tiled=True)


def shift(array, by):
    return lax.ppermute(array, "q", [(k, (k + by) % RING) for k in range(RING)])


def kernel(body, out_shape, given=(), scratch=()):
    specs = [pl.BlockSpec(memory_space=space) for space in given]

    def call(*operands):
        rest = operands[len(specs) :]
        held = [pltpu.with_memory_space_constraint(array, pltpu.VMEM) for array in rest]
        return pl.pallas_call(
            body,
            out_shape=out_shape,
            in_specs=specs + [pl.BlockSpec(memory_space=pltpu.VMEM)] * len(held),
            scratch_shapes=scratch,
        )(*operands[: len(specs)], *held)

    return call


def block_step(expression, current, next_packed, covariates):
    rows, genes = expression.shape
    variants = current.shape[1]
    covs = covariates.shape[1]
    held, words = next_packed.shape
    share = words // RING
    total = rows * RING * LOCAL
    own_genes = genes // (RING * LOCAL)
    q = lax.axis_index("q")
    j = lax.axis_index("j")

    count = RING * held
    height = count + 8 + covs // 2
    half_genes = genes // LOCAL // 2
    at = half_genes + variants
    moved, packed = kernel(
        first_kernel,
        (
            jax.ShapeDtypeStruct((LOCAL * rows, at + 2 * covs), BF16),
            pltpu.VMEM((RING * 8, 128), jnp.int32),
        ),
        [pltpu.VMEM] * 4,
    )(expression, current, covariates, next_packed)
    moved = exchange(moved, "j")
    others = kernel(
        second_kernel, jax.ShapeDtypeStruct((LOCAL * rows, half_genes), BF16), [pltpu.VMEM]
    )(expression)
    others = exchange(others, "j")
    packed = packed.reshape(RING, 8, 128)
    pieces = []
    for ahead in range(RING):
        piece = lax.dynamic_index_in_dim(packed, (q + ahead) % RING, 0, keepdims=False)
        pieces.append(shift(piece, ahead) if ahead else piece)

    where = jnp.stack([j, q]).astype(jnp.int32)
    half = own_genes // 2

    def product(array):
        return kernel(
            functools.partial(product_kernel, half_genes, variants, half_genes),
            [pltpu.VMEM((half, variants), F32)] * RING,
            [pltpu.SMEM],
            [pltpu.VMEM((half_genes, variants), F32)],
        )(where, array, moved)

    blocks = (product(moved), product(others))

    stats = kernel(
        functools.partial(stats_kernel, held, share, at, covs),
        jax.ShapeDtypeStruct((height, 2 * covs), F32),
        [pltpu.SMEM],
    )(where, moved, *pieces)
    sums = [stats]
    ahead, behind = stats, stats
    for hop in range(1, RING // 2 + 1):
        ahead = shift(ahead, 1)
        sums.append(ahead)
        if hop < RING // 2:
            behind = shift(behind, -1)
            sums.append(behind)
    placed = kernel(
        functools.partial(finish_kernel, held, share, at, variants, covs, float(total)),
        jax.ShapeDtypeStruct((LOCAL * rows, variants), BF16),
        [pltpu.SMEM],
    )(where, moved, *pieces, *sums)
    placed = exchange(placed, "j")
    next_block = jnp.sum(placed.reshape(LOCAL, rows, variants).astype(F32), axis=0).astype(BF16)

    scale_factor = float(total) ** (-0.5)
    far = RING // 2
    carried = {}
    for step in range(1, far + 1):
        for name, way, part, late in STREAMS:
            if step + late <= far:
                block = blocks[part][way * (far + 1 - step - late) % RING]
                held_sum = carried[name] + block if name in carried else block
                carried[name] = shift(held_sum, way)
    scores = kernel(
        functools.partial(total_kernel, scale_factor),
        jax.ShapeDtypeStruct((own_genes, variants), F32),
    )(blocks[0][0], blocks[1][0], *(carried[name] for name in ("right_a", "right_b", "left_a", "left_b")))
    return (scores, next_block)


STREAMS = (("right_a", 1, 0, 0), ("left_b", -1, 1, 0), ("right_b", 1, 1, 1), ("left_a", -1, 0, 1))


def solution(mesh):
    split = Mesh(mesh.devices.reshape(mesh.shape["parts"], RING, LOCAL), ("parts", "q", "j"))
    return jax.shard_map(
        block_step, mesh=split, in_specs=(SPEC,) * 4, out_specs=(SPEC,) * 2, check_vma=False
    )
```

```python
import functools

import jax
import jax.numpy as jnp
from jax import lax
from jax.experimental import pallas as pl
from jax.experimental.pallas import tpu as pltpu
from jax.sharding import Mesh
from jax.sharding import PartitionSpec as P

RING = 8
LOCAL = 16
SPEC = P(("parts", "q", "p", "c"), None)
NEAR = ("p", "c")
F32 = jnp.float32
BF16 = jnp.bfloat16
HIGHEST = lax.Precision.HIGHEST
WORD = 16
PIECES = RING // 2 + 2
ROOM = pltpu.CompilerParams(vmem_limit_bytes=16 * 2**20)


def core():
    return lax.axis_index("c")


def position():
    return lax.axis_index("q")


def one_hot(hits):
    return hits.astype(F32).astype(BF16)


def dot(left, right, dims, precision=None):
    return lax.dot_general(
        left, right, (dims, ((), ())), precision=precision, preferred_element_type=F32
    )


def prepare_kernel(expression_ref, current_ref, covariates_ref, out_ref):
    rows, genes = expression_ref.shape
    block = genes // RING
    share = block // LOCAL
    half = share // 2
    far = RING // 2
    around = []
    for ahead in range(RING):
        at = pl.multiple_of(lax.rem(position() + ahead, RING) * block, 128)
        around.append(expression_ref[:, pl.ds(at, block)])
    cov = covariates_ref[...]
    high = cov.astype(BF16)
    low = (cov - high.astype(F32)).astype(BF16)
    own = [current_ref[...], high, low]
    for j in range(LOCAL):
        way = 1 - 2 * (j % 2)
        pieces = []
        for target in (j ^ 1, j):
            at = target * share + (j % 2) * half
            pieces.append(around[far][:, at : at + half])
        for distance in range(far - 1, 0, -1):
            for target in (j ^ 1, j):
                at = target * share
                halves = [
                    around[way * distance % RING][:, at + part * half : at + (part + 1) * half]
                    for part in (j % 2, 1 - j % 2)
                ]
                pieces += halves
        pieces.append(around[0][:, j * share : (j + 1) * share])
        out_ref[j * rows : (j + 1) * rows, :] = jnp.concatenate(pieces + own, axis=1)


def words_kernel(mine_ref, given_ref, out_ref):
    held, words = mine_ref.shape
    split = words // RING
    first = core() == 0
    mine, given = mine_ref[...], given_ref[...]
    both = jnp.concatenate(
        [jnp.where(first, mine, given), jnp.where(first, given, mine)], axis=0
    )
    out_ref[...] = jnp.zeros_like(out_ref)
    for q in range(RING):
        out_ref[q * 8 : q * 8 + 2 * held, 0:split] = both[:, q * split : (q + 1) * split]


def product_kernel(genes, variants, rows_ref, *refs):
    whole = dot(rows_ref[:, :genes], rows_ref[:, genes : genes + variants], ((0,), (0,)))
    refs[0][...] = rows_ref[:, genes + variants :]
    at = 0
    for ref in refs[1:]:
        ref[...] = whole[at : at + ref.shape[0], :]
        at += ref.shape[0]


def merge_kernel(block_ref, come_ref, out_ref):
    half = come_ref.shape[0]
    out_ref[0:half, :] = block_ref[0:half, :] + come_ref[...]
    out_ref[half:, :] = block_ref[half:, :]


def total_kernel(scale, own_ref, mine_ref, given_ref, out_ref):
    half = own_ref.shape[0] // 2
    here = core()
    for part in range(2):
        rows = slice(part * half, (part + 1) * half)
        mine = mine_ref[pl.ds((here ^ part) * half, half), :]
        given = given_ref[pl.ds((here ^ part ^ 1) * half, half), :]
        out_ref[rows, :] = (own_ref[rows, :] + mine + given) * scale


def unpack(word_refs, held, share):
    rows = [ref[at : at + held, 0:share] for ref in word_refs for at in range(0, ref.shape[0], 8)]
    words = jnp.concatenate(rows, axis=0)
    wide = jnp.concatenate([words] * 4, axis=1)
    lane = lax.broadcasted_iota(jnp.int32, wide.shape, 1)
    octets = (lax.shift_right_logical(wide, 8 * (lane // share)) & 255).astype(F32).astype(BF16)
    count = RING * held
    row = lax.broadcasted_iota(jnp.int32, (count, count), 0)
    col = lax.broadcasted_iota(jnp.int32, (count, count), 1)
    behind = (position() - row // held) * (1 - 2 * core()) % RING
    slot = jnp.where(behind <= RING // 2, behind, RING + RING // 2 - behind)
    order = (col // held == slot) & (col % held == row % held)
    octets = dot(order.astype(F32).astype(BF16), octets, ((1,), (0,))).astype(BF16)
    samples = share * WORD
    row = lax.broadcasted_iota(jnp.int32, (4 * share, samples), 0)
    col = lax.broadcasted_iota(jnp.int32, (4 * share, samples), 1)
    pick = (row % share == col // WORD) & (row // share == (col % WORD) // 4)
    spread = dot(octets, pick.astype(F32).astype(BF16), ((1,), (0,))).astype(jnp.int32)
    place = lax.broadcasted_iota(jnp.int32, spread.shape, 1)
    return (lax.shift_right_logical(spread, 2 * (place % 4)) & 3).astype(F32)


def covariate_terms(rows_ref, covs):
    return [rows_ref[:, k * covs : (k + 1) * covs] for k in range(2)]


def stats_kernel(held, share, covs, rows_ref, *refs):
    out_ref = refs[PIECES]
    dosage = unpack(refs[:PIECES], held, share)
    count, samples = dosage.shape
    ones = jnp.ones((8, samples), F32)
    wide = jnp.concatenate([dosage, ones], axis=0)
    exact = wide.astype(BF16)
    terms = covariate_terms(rows_ref, covs)
    projected = sum(dot(exact, term, ((1,), (0,))) for term in reversed(terms))
    half = covs // 2
    height = count + 8 + half
    cov = sum(term.astype(F32) for term in reversed(terms))
    gram = dot(cov, cov, ((0,), (0,)), HIGHEST)
    counted = jnp.sum(wide, axis=1, keepdims=True)
    squares = jnp.sum(wide * wide, axis=1, keepdims=True)
    pad = jnp.zeros((count + 8, covs - 2), F32)
    table = jnp.concatenate([projected, counted, squares, pad], axis=1)
    lower = jnp.concatenate([gram[0:half], gram[half:]], axis=1)
    out_ref[0 : count + 8, :] = table
    out_ref[count + 8 : height, :] = lower


def one_way_kernel(*refs):
    last = jnp.where(core() == 0, refs[-2][...], 0.0)
    refs[-1][...] = sum((ref[...] for ref in refs[:-2]), last)


def finish_kernel(held, share, variants, covs, total, rows_ref, *refs):
    out_ref, placed_ref = refs[-2:]
    dosage = unpack(refs[:PIECES], held, share)
    count, _ = dosage.shape
    half = covs // 2
    table = refs[PIECES][...]
    for ref in refs[PIECES + 1 : -2]:
        table = table + ref[...]
    gram = jnp.concatenate(
        [
            table[count + 8 : count + 8 + half, 0:covs],
            table[count + 8 : count + 8 + half, covs : 2 * covs],
        ],
        axis=0,
    )
    projected = table[0:count, 0:covs]
    cov_sums = table[count : count + 1, 0:covs]
    counted = table[0:count, covs : covs + 1]
    squares = table[0:count, covs + 1 : covs + 2]
    average = counted / total
    loading = projected - average * cov_sums
    through = dot(loading, gram, ((1,), (0,)), HIGHEST)
    sq_norm = (
        squares
        - counted * average
        + jnp.sum(loading * (through - 2.0 * loading), axis=1, keepdims=True)
    )
    cov = sum(term.astype(F32) for term in reversed(covariate_terms(rows_ref, covs)))
    leftover = dosage - average - dot(loading, cov, ((1,), (1,)), HIGHEST)
    scaled = (leftover * lax.rsqrt(sq_norm / total + 1e-05)).astype(BF16)
    row = lax.broadcasted_iota(jnp.int32, (count, variants), 0)
    col = lax.broadcasted_iota(jnp.int32, (count, variants), 1)
    target = (row // held) * (held * LOCAL // 2) + lax.axis_index("p") * held + row % held
    placed_ref[...] = dot(scaled, one_hot(col == target), ((0,), (0,)))
    share_rows = scaled.shape[1] // LOCAL
    for peer in range(LOCAL // 2):
        first = pl.multiple_of((2 * peer + core()) * share_rows, share_rows)
        out_ref[peer * share_rows : (peer + 1) * share_rows, :] = placed_ref[
            pl.ds(first, share_rows), :
        ].astype(BF16)


def exchange(array, axis):
    return lax.all_to_all(array, axis, split_axis=0, concat_axis=0, tiled=True)


def hop(array, steps=1):
    pairs = [
        (2 * k + side, 2 * ((k + steps * (1 - 2 * side)) % RING) + side)
        for k in range(RING)
        for side in range(2)
    ]
    return lax.ppermute(array, ("q", "c"), pairs)


def swap(array):
    return lax.ppermute(array, "c", [(0, 1), (1, 0)])


def kernel(body, out_shape, given=(), scratch=()):
    specs = [pl.BlockSpec(memory_space=space) for space in given]

    def call(*operands):
        rest = operands[len(specs) :]
        held = [pltpu.with_memory_space_constraint(array, pltpu.VMEM) for array in rest]
        return pl.pallas_call(
            body,
            out_shape=out_shape,
            compiler_params=None if given else ROOM,
            in_specs=specs + [pl.BlockSpec(memory_space=pltpu.VMEM)] * len(held),
            scratch_shapes=scratch,
        )(*operands[: len(specs)], *held)

    return call


def block_step(expression, current, next_packed, covariates):
    rows, genes = expression.shape
    variants = current.shape[1]
    covs = covariates.shape[1]
    held, words = 2 * next_packed.shape[0], next_packed.shape[1]
    share = words // RING
    total = rows * RING * LOCAL
    own_genes = genes // (RING * LOCAL)
    q = lax.axis_index("q")

    count = RING * held
    height = count + 8 + covs // 2
    local_genes = genes // LOCAL
    at = local_genes + variants
    moved = kernel(
        prepare_kernel, jax.ShapeDtypeStruct((LOCAL * rows, at + 2 * covs), BF16), [pltpu.VMEM] * 3
    )(expression, current, covariates)
    moved = exchange(moved, NEAR)
    packed = kernel(
        words_kernel, pltpu.VMEM((RING * 8, 128), jnp.int32), [pltpu.VMEM]
    )(next_packed, swap(next_packed))
    packed = packed.reshape(RING, 8, 128)
    far = RING // 2
    way = 1 - 2 * lax.axis_index("c")
    mine = []
    for distance in range(1, far + 1):
        piece = lax.dynamic_index_in_dim(
            packed, (q + way * distance + RING) % RING, 0, keepdims=False
        )
        mine.append(hop(piece, distance))
    given = swap(jnp.concatenate(mine[:-1], axis=0))
    pieces = [lax.dynamic_index_in_dim(packed, q, 0, keepdims=False), *mine, given]

    heights = [own_genes // 2] * 2 + [own_genes] * (2 * far - 1)
    terms, *blocks = kernel(
        functools.partial(product_kernel, local_genes, variants),
        [pltpu.VMEM((LOCAL * rows, 2 * covs), BF16)]
        + [pltpu.VMEM((height, variants), F32) for height in heights[:-1]]
        + [jax.ShapeDtypeStruct((own_genes, variants), F32)],
    )(moved)

    stats = kernel(
        functools.partial(stats_kernel, held, share, covs),
        jax.ShapeDtypeStruct((height, 2 * covs), F32),
    )(terms, *pieces)
    passed = []
    ahead = stats
    for _ in range(1, RING // 2 + 1):
        ahead = hop(ahead)
        passed.append(ahead)
    one_way = kernel(one_way_kernel, pltpu.VMEM((height, 2 * covs), F32))(*passed)
    sums = [stats, one_way, swap(one_way)]
    placed = kernel(
        functools.partial(finish_kernel, held, share, variants, covs, float(total)),
        jax.ShapeDtypeStruct((LOCAL // 2 * rows, variants), BF16),
        scratch=[pltpu.VMEM((LOCAL * rows, variants), F32)],
    )(terms, *pieces, *sums)
    placed = exchange(placed, "p")
    next_block = jnp.sum(placed.reshape(-1, rows, variants).astype(F32), axis=0).astype(BF16)

    scale_factor = float(total) ** (-0.5)
    merged = pltpu.VMEM((own_genes, variants), F32)
    away, same = hop(blocks[0]), hop(blocks[1])
    away = hop(kernel(merge_kernel, merged)(blocks[2], away))
    same = hop(kernel(merge_kernel, merged)(blocks[3], same))
    for step in range(3, far + 1):
        away = hop(blocks[2 * step - 2] + away)
        same = hop(blocks[2 * step - 1] + same)
    given = swap(away)
    scores = kernel(
        functools.partial(total_kernel, scale_factor),
        jax.ShapeDtypeStruct((own_genes, variants), F32),
    )(blocks[-1], same, given)
    return (scores, next_block)


def solution(mesh):
    split = Mesh(mesh.devices.reshape(mesh.shape["parts"], RING, LOCAL // 2, 2), ("parts", "q", "p", "c"))
    return jax.shard_map(
        block_step, mesh=split, in_specs=(SPEC,) * 4, out_specs=(SPEC,) * 2, check_vma=False
    )
```

```python
import functools

import jax
import jax.numpy as jnp
from jax import lax
from jax.experimental import pallas as pl
from jax.experimental.pallas import tpu as pltpu
from jax.sharding import Mesh
from jax.sharding import PartitionSpec as P

RING = 8
LOCAL = 16
SPEC = P(("parts", "q", "p", "c"), None)
NEAR = ("p", "c")
F32 = jnp.float32
BF16 = jnp.bfloat16
HIGHEST = lax.Precision.HIGHEST
WORD = 16
ROOM = pltpu.CompilerParams(vmem_limit_bytes=16 * 2**20)


def core():
    return lax.axis_index("c")


def position():
    return lax.axis_index("q")


def one_hot(hits):
    return hits.astype(F32).astype(BF16)


def dot(left, right, dims, precision=None):
    return lax.dot_general(
        left, right, (dims, ((), ())), precision=precision, preferred_element_type=F32
    )


def prepare_kernel(expression_ref, current_ref, covariates_ref, out_ref):
    rows, genes = expression_ref.shape
    block = genes // RING
    share = block // LOCAL
    half = share // 2
    far = RING // 2
    around = []
    for ahead in range(RING):
        at = pl.multiple_of(lax.rem(position() + ahead, RING) * block, 128)
        around.append(expression_ref[:, pl.ds(at, block)])
    cov = covariates_ref[...]
    high = cov.astype(BF16)
    low = (cov - high.astype(F32)).astype(BF16)
    own = [current_ref[...], high, low]
    for j in range(LOCAL):
        way = 1 - 2 * (j % 2)
        pieces = []
        for target in (j ^ 1, j):
            at = target * share + (j % 2) * half
            pieces.append(around[far][:, at : at + half])
        for distance in range(far - 1, 0, -1):
            for target in (j ^ 1, j):
                at = target * share
                there = around[way * distance % RING]
                cuts = ((at, at + half), (at + half, at + share))
                if j % 2:
                    pieces += [there[:, first:last] for first, last in reversed(cuts)]
                else:
                    pieces.append(there[:, at : at + share])
        pieces.append(around[0][:, j * share : (j + 1) * share])
        out_ref[j * rows : (j + 1) * rows, :] = jnp.concatenate(pieces + own, axis=1)


def words_kernel(mine_ref, given_ref, out_ref):
    held, words = mine_ref.shape
    split = words // RING
    first = core() == 0
    mine, given = mine_ref[...], given_ref[...]
    both = jnp.concatenate(
        [jnp.where(first, mine, given), jnp.where(first, given, mine)], axis=0
    )
    out_ref[...] = jnp.zeros_like(out_ref)
    for q in range(RING):
        out_ref[q * 8 : q * 8 + 2 * held, 0:split] = both[:, q * split : (q + 1) * split]


def product_kernel(genes, variants, rows_ref, *refs):
    whole = dot(rows_ref[:, :genes], rows_ref[:, genes : genes + variants], ((0,), (0,)))
    refs[0][...] = rows_ref[:, genes + variants :]
    at = 0
    for ref in refs[1:]:
        ref[...] = whole[at : at + ref.shape[0], :]
        at += ref.shape[0]


def merge_kernel(block_ref, come_ref, out_ref):
    half = come_ref.shape[0]
    out_ref[0:half, :] = block_ref[0:half, :] + come_ref[...]
    out_ref[half:, :] = block_ref[half:, :]


def total_kernel(scale, own_ref, mine_ref, given_ref, out_ref):
    half = own_ref.shape[0] // 2
    here = core()
    for part in range(2):
        rows = slice(part * half, (part + 1) * half)
        mine = mine_ref[pl.ds((here ^ part) * half, half), :]
        given = given_ref[pl.ds((here ^ part ^ 1) * half, half), :]
        out_ref[rows, :] = (own_ref[rows, :] + mine + given) * scale


def unpack(word_refs, held, share):
    words = jnp.concatenate([ref[0:held, 0:share] for ref in word_refs], axis=0)
    wide = jnp.concatenate([words] * 4, axis=1)
    lane = lax.broadcasted_iota(jnp.int32, wide.shape, 1)
    octets = (lax.shift_right_logical(wide, 8 * (lane // share)) & 255).astype(F32).astype(BF16)
    count = RING * held
    row = lax.broadcasted_iota(jnp.int32, (count, count), 0)
    col = lax.broadcasted_iota(jnp.int32, (count, count), 1)
    behind = (position() + RING - row // held) % RING
    order = (col // held == behind) & (col % held == row % held)
    octets = dot(order.astype(F32).astype(BF16), octets, ((1,), (0,))).astype(BF16)
    samples = share * WORD
    row = lax.broadcasted_iota(jnp.int32, (4 * share, samples), 0)
    col = lax.broadcasted_iota(jnp.int32, (4 * share, samples), 1)
    pick = (row % share == col // WORD) & (row // share == (col % WORD) // 4)
    spread = dot(octets, pick.astype(F32).astype(BF16), ((1,), (0,))).astype(jnp.int32)
    place = lax.broadcasted_iota(jnp.int32, spread.shape, 1)
    return (lax.shift_right_logical(spread, 2 * (place % 4)) & 3).astype(F32)


def covariate_terms(rows_ref, covs):
    return [rows_ref[:, k * covs : (k + 1) * covs] for k in range(2)]


def stats_kernel(held, share, covs, rows_ref, *refs):
    out_ref = refs[RING]
    dosage = unpack(refs[:RING], held, share)
    count, samples = dosage.shape
    ones = jnp.ones((8, samples), F32)
    wide = jnp.concatenate([dosage, ones], axis=0)
    exact = wide.astype(BF16)
    terms = covariate_terms(rows_ref, covs)
    projected = sum(dot(exact, term, ((1,), (0,))) for term in reversed(terms))
    half = covs // 2
    height = count + 8 + half
    cov = sum(term.astype(F32) for term in reversed(terms))
    gram = dot(cov, cov, ((0,), (0,)), HIGHEST)
    counted = jnp.sum(wide, axis=1, keepdims=True)
    squares = jnp.sum(wide * wide, axis=1, keepdims=True)
    pad = jnp.zeros((count + 8, covs - 2), F32)
    table = jnp.concatenate([projected, counted, squares, pad], axis=1)
    lower = jnp.concatenate([gram[0:half], gram[half:]], axis=1)
    out_ref[0 : count + 8, :] = table
    out_ref[count + 8 : height, :] = lower


def one_way_kernel(*refs):
    last = jnp.where(core() == 0, refs[-2][...], 0.0)
    refs[-1][...] = sum((ref[...] for ref in refs[:-2]), last)


def finish_kernel(held, share, variants, covs, total, rows_ref, *refs):
    out_ref, placed_ref = refs[-2:]
    dosage = unpack(refs[:RING], held, share)
    count, _ = dosage.shape
    half = covs // 2
    table = refs[RING][...]
    for ref in refs[RING + 1 : -2]:
        table = table + ref[...]
    gram = jnp.concatenate(
        [
            table[count + 8 : count + 8 + half, 0:covs],
            table[count + 8 : count + 8 + half, covs : 2 * covs],
        ],
        axis=0,
    )
    projected = table[0:count, 0:covs]
    cov_sums = table[count : count + 1, 0:covs]
    counted = table[0:count, covs : covs + 1]
    squares = table[0:count, covs + 1 : covs + 2]
    average = counted / total
    loading = projected - average * cov_sums
    through = dot(loading, gram, ((1,), (0,)), HIGHEST)
    sq_norm = (
        squares
        - counted * average
        + jnp.sum(loading * (through - 2.0 * loading), axis=1, keepdims=True)
    )
    cov = sum(term.astype(F32) for term in reversed(covariate_terms(rows_ref, covs)))
    leftover = dosage - average - dot(loading, cov, ((1,), (1,)), HIGHEST)
    scaled = (leftover * lax.rsqrt(sq_norm / total + 1e-05)).astype(BF16)
    row = lax.broadcasted_iota(jnp.int32, (count, variants), 0)
    col = lax.broadcasted_iota(jnp.int32, (count, variants), 1)
    target = (row // held) * (held * LOCAL // 2) + lax.axis_index("p") * held + row % held
    placed_ref[...] = dot(scaled, one_hot(col == target), ((0,), (0,)))
    share_rows = scaled.shape[1] // LOCAL
    for peer in range(LOCAL // 2):
        first = pl.multiple_of((2 * peer + core()) * share_rows, share_rows)
        out_ref[peer * share_rows : (peer + 1) * share_rows, :] = placed_ref[
            pl.ds(first, share_rows), :
        ].astype(BF16)


def exchange(array, axis):
    return lax.all_to_all(array, axis, split_axis=0, concat_axis=0, tiled=True)


def shift(array, by):
    return lax.ppermute(array, "q", [(k, (k + by) % RING) for k in range(RING)])


def hop(array):
    pairs = [
        (2 * k + core, 2 * ((k + 1 - 2 * core) % RING) + core)
        for k in range(RING)
        for core in range(2)
    ]
    return lax.ppermute(array, ("q", "c"), pairs)


def swap(array):
    return lax.ppermute(array, "c", [(0, 1), (1, 0)])


def kernel(body, out_shape, given=(), scratch=()):
    specs = [pl.BlockSpec(memory_space=space) for space in given]

    def call(*operands):
        rest = operands[len(specs) :]
        held = [pltpu.with_memory_space_constraint(array, pltpu.VMEM) for array in rest]
        return pl.pallas_call(
            body,
            out_shape=out_shape,
            compiler_params=None if given else ROOM,
            in_specs=specs + [pl.BlockSpec(memory_space=pltpu.VMEM)] * len(held),
            scratch_shapes=scratch,
        )(*operands[: len(specs)], *held)

    return call


def block_step(expression, current, next_packed, covariates):
    rows, genes = expression.shape
    variants = current.shape[1]
    covs = covariates.shape[1]
    held, words = 2 * next_packed.shape[0], next_packed.shape[1]
    share = words // RING
    total = rows * RING * LOCAL
    own_genes = genes // (RING * LOCAL)
    q = lax.axis_index("q")

    count = RING * held
    height = count + 8 + covs // 2
    local_genes = genes // LOCAL
    at = local_genes + variants
    moved = kernel(
        prepare_kernel, jax.ShapeDtypeStruct((LOCAL * rows, at + 2 * covs), BF16), [pltpu.VMEM] * 3
    )(expression, current, covariates)
    moved = exchange(moved, NEAR)
    packed = kernel(
        words_kernel, pltpu.VMEM((RING * 8, 128), jnp.int32), [pltpu.VMEM]
    )(next_packed, swap(next_packed))
    packed = packed.reshape(RING, 8, 128)
    pieces = []
    for ahead in range(RING):
        piece = lax.dynamic_index_in_dim(packed, (q + ahead) % RING, 0, keepdims=False)
        pieces.append(shift(piece, ahead) if ahead else piece)

    far = RING // 2
    heights = [own_genes // 2] * 2 + [own_genes] * (2 * far - 1)
    terms, *blocks = kernel(
        functools.partial(product_kernel, local_genes, variants),
        [pltpu.VMEM((LOCAL * rows, 2 * covs), BF16)]
        + [pltpu.VMEM((height, variants), F32) for height in heights[:-1]]
        + [jax.ShapeDtypeStruct((own_genes, variants), F32)],
    )(moved)

    stats = kernel(
        functools.partial(stats_kernel, held, share, covs),
        jax.ShapeDtypeStruct((height, 2 * covs), F32),
    )(terms, *pieces)
    passed = []
    ahead = stats
    for _ in range(1, RING // 2 + 1):
        ahead = hop(ahead)
        passed.append(ahead)
    one_way = kernel(one_way_kernel, pltpu.VMEM((height, 2 * covs), F32))(*passed)
    sums = [stats, one_way, swap(one_way)]
    placed = kernel(
        functools.partial(finish_kernel, held, share, variants, covs, float(total)),
        jax.ShapeDtypeStruct((LOCAL // 2 * rows, variants), BF16),
        scratch=[pltpu.VMEM((LOCAL * rows, variants), F32)],
    )(terms, *pieces, *sums)
    placed = exchange(placed, "p")
    next_block = jnp.sum(placed.reshape(-1, rows, variants).astype(F32), axis=0).astype(BF16)

    scale_factor = float(total) ** (-0.5)
    merged = pltpu.VMEM((own_genes, variants), F32)
    away, same = hop(blocks[0]), hop(blocks[1])
    away = hop(kernel(merge_kernel, merged)(blocks[2], away))
    same = hop(kernel(merge_kernel, merged)(blocks[3], same))
    for step in range(3, far + 1):
        away = hop(blocks[2 * step - 2] + away)
        same = hop(blocks[2 * step - 1] + same)
    given = swap(away)
    scores = kernel(
        functools.partial(total_kernel, scale_factor),
        jax.ShapeDtypeStruct((own_genes, variants), F32),
    )(blocks[-1], same, given)
    return (scores, next_block)


def solution(mesh):
    split = Mesh(mesh.devices.reshape(mesh.shape["parts"], RING, LOCAL // 2, 2), ("parts", "q", "p", "c"))
    return jax.shard_map(
        block_step, mesh=split, in_specs=(SPEC,) * 4, out_specs=(SPEC,) * 2, check_vma=False
    )
```
